32 devices in a mesh: gx: 8 (over y, x, core), gy: 4 (over z).
Axes of the slice: x: 2, y: 2, z: 4, core: 2. Of those that a mesh axis runs over, the one named last changes fastest.
Arguments:
- products: bfloat16 [1536, 3, 2048], P('gy', None, 'gx'), may hold values from -6 to 6
- operator: bfloat16 [1536, 1536], P(None, 'gy'), may hold values from -0.21875 to 0.21875
Outputs:
- derivative: bfloat16 [1536, 3, 2048], P(('gy', 'gx'))
The draws below stay inside these ranges and needn't reach their ends.
All inputs are finite; a program needn't handle non-finite values.
Results may differ from the reference program's by a relative error of at most 0.002.
Values may be sent and summed in bfloat16 or wider, within the bound.
No kernel may reach another device: no remote copies, remote signals or barrier semaphores. Data moves between devices by JAX's collectives and lax.ppermute only.
A program may use at most 64 MiB of HBM per device.

```python
import jax
import jax.numpy as jnp

NY = 1536
MODES = 2048


def strengthened(array, own_key, source, target, blocks, factor):
    owner, partner = [(jnp.arange(array.shape[position]) // (array.shape[position] // blocks)).reshape([-1 if axis == position else 1 for axis in range(array.ndim)]) for position in (source, target)]
    chosen = jax.random.permutation(own_key, blocks)[partner]
    strong = (owner == chosen) | (owner == (partner + blocks // 2) % blocks)
    return jnp.where(strong, factor * array, array)


def block_scale(rng, shape, pieces, smallest, largest):
    loudness = 1.0
    for axis_at, shards_of in pieces:
        heights = jax.random.uniform(jax.random.fold_in(jax.random.fold_in(rng, 6), axis_at), (shards_of,), jnp.float32, smallest / len(pieces), largest / len(pieces))
        loudness = loudness * jnp.repeat(jnp.exp(heights), shape[axis_at] // shards_of).reshape((-1,) + (1,) * (len(shape) - 1 - axis_at))
    return loudness


def gaussian(own_key, extent, scale, limit, split=(), kind=jnp.bfloat16):
    entries = scale * jax.random.normal(own_key, extent, jnp.float32)
    if split:
        entries = entries * block_scale(own_key, extent, split, -0.22, 0.18)
    return jnp.clip(entries, -limit, limit).astype(kind)


def heavy_noise(key, shape, width, limit, pieces, heavy, kind=jnp.bfloat16):
    entries = width * jax.random.normal(key, shape, jnp.float32)
    if pieces:
        entries = entries * block_scale(key, shape, pieces, -0.22, 0.18)
    return jnp.clip(strengthened(entries, jax.random.fold_in(key, 3), *heavy), -limit, limit).astype(kind)


def setup_inputs(seed: int = 0) -> dict:
    streams_of = jax.random.split(jax.random.key(seed), 3)
    products = gaussian(streams_of[0], (NY, 3, MODES), 1.0, 6.0, ((0, 4), (2, 8)))
    operator = heavy_noise(streams_of[1], (NY, NY), NY ** -0.5, 0.21875, ((1, 4),), (1, 0, 4, 2.0))
    return dict(products=products, operator=operator)


def reference(products, operator):
    flat = products.reshape(NY, 3 * MODES)
    summed = jnp.dot(operator, flat, preferred_element_type=jnp.float32)
    return summed.astype(jnp.bfloat16).reshape(NY, 3, MODES)
```

```python
import jax
import jax.numpy as jnp
from jax import lax
from jax.experimental import pallas as pl
from jax.experimental.pallas import tpu as pltpu
from jax.sharding import PartitionSpec as P


def hop(index, step, size):
    return index ^ step if size & (size - 1) == 0 else (index + step) % size


def back(index, step, size):
    return index ^ step if size & (size - 1) == 0 else (index - step + size) % size


def assemble(place, *refs):
    *parts, out = refs
    half = out.shape[2] // (2 * len(parts))
    for number, part in enumerate(parts):
        for other in range(2):
            start = pl.multiple_of(place[2 * number + other] * half, half)
            for comp in range(out.shape[0]):
                column = (other * out.shape[0] + comp) * half
                out[comp, :, pl.ds(start, half)] = part[:, column : column + half]


def direct(products, operator):
    points, comps, modes = products.shape
    flat = products.reshape(points, comps * modes)
    partial = jnp.dot(operator, flat, preferred_element_type=jnp.float32)
    summed = lax.psum_scatter(partial, "gy", scatter_dimension=0, tiled=True)
    result = summed.astype(jnp.bfloat16).reshape(points, comps, modes)
    return lax.all_to_all(result, "gx", split_axis=0, concat_axis=2, tiled=True)


def paired(wide, deep, products, operator):
    points, comps, modes = products.shape
    chips, half = wide // 2, modes // 2
    piece = points // chips
    x, z = lax.axis_index("gx"), lax.axis_index("gy")
    chip, core, q = x // 2, x % 2, z % 2
    pair = z - q

    shares = []
    for k in range(1, deep):
        target = hop(z, k, deep)
        start = (target - target % 2 + core) * points + chip * piece
        share = lax.dynamic_slice_in_dim(operator, start, piece, 0)
        shares.append(lax.ppermute(share, "gy", [(i, hop(i, k, deep)) for i in range(deep)]))
    arrived = jnp.stack(shares)

    halves = [
        lax.dynamic_slice_in_dim(products, (q ^ odd) * half, half, 2).reshape(points, comps * half)
        for odd in range(2)
    ]
    mine = [halves[0]]
    for k in range(deep - 1, 0, -1):
        mine.insert(1, lax.ppermute(halves[k % 2], "gy", [(i, hop(i, k, deep)) for i in range(deep)]))

    gathered = [arrived]
    for j in range(1, chips):
        pairs = [(i, 2 * hop(i // 2, j, chips) + i % 2) for i in range(wide)]
        gathered.append(lax.ppermute(arrived, "gx", pairs))
    own = [
        lax.dynamic_slice_in_dim(operator, (pair + core) * points + back(chip, j, chips) * piece, piece, 0)
        for j in range(chips)
    ]
    weights = [jnp.concatenate(own)]
    for k in range(1, deep):
        weights.append(jnp.concatenate([g[k - 1] for g in gathered]))

    swap = [(i, i ^ 1) for i in range(wide)]
    total = 0.0
    for k in [0] + list(range(1, deep)):
        both = jnp.concatenate([mine[k], lax.ppermute(mine[k], "gx", swap)], axis=1)
        total = total + jnp.dot(weights[k], both, preferred_element_type=jnp.float32)
    result = total.astype(jnp.bfloat16).reshape(chips, 2, piece // 2, 2 * comps * half)

    received, places = [], []
    for j in range(chips):
        for t in range(2):
            part = lax.dynamic_index_in_dim(result[j], q ^ t, 0, keepdims=False)
            pairs = []
            for i in range(wide):
                for y in range(deep):
                    to = 2 * back(i // 2, j, chips) + (y % 2 ^ t)
                    pairs.append((i * deep + y, to * deep + y - y % 2 + i % 2))
            received.append(lax.ppermute(part, ("gx", "gy"), pairs))
            source = hop(chip, j, chips)
            for e in range(2):
                places.append((source * 2 + (q ^ e)) * 2 + (core ^ t))

    out = pl.pallas_call(
        assemble,
        out_shape=jax.ShapeDtypeStruct((comps, piece // 2, wide * modes), jnp.bfloat16),
        in_specs=[pl.BlockSpec(memory_space=pltpu.SMEM)]
        + [pl.BlockSpec(memory_space=pltpu.VMEM)] * len(received),
        out_specs=pl.BlockSpec(memory_space=pltpu.VMEM),
    )(jnp.stack(places).astype(jnp.int32), *received)
    return out.transpose(1, 0, 2)


def solution(mesh):
    wide, deep = mesh.shape["gx"], mesh.shape["gy"]

    def body(products, operator):
        if wide % 2 or deep % 2:
            return direct(products, operator)
        return paired(wide, deep, products, operator)

    return jax.shard_map(
        body,
        mesh=mesh,
        in_specs=(P("gy", None, "gx"), P(None, "gy")),
        out_specs=P(("gy", "gx"), None, None),
        check_vma=False,
    )
```

```python
import jax
import jax.numpy as jnp
from jax import lax
from jax.experimental import pallas as pl
from jax.experimental.pallas import tpu as pltpu
from jax.sharding import PartitionSpec as P


def hop(index, step, size):
    return index ^ step if size & (size - 1) == 0 else (index + step) % size


def back(index, step, size):
    return index ^ step if size & (size - 1) == 0 else (index - step + size) % size


def assemble(first, place, *refs):
    *parts, _, out, whole, sem = refs
    comps, _, width = whole.shape
    half = width // (2 * len(parts))
    for number, part in enumerate(parts):
        for other in range(2):
            start = pl.multiple_of(place[2 * number + other] * half, half)
            for comp in range(comps):
                column = (other * comps + comp) * half
                whole[comp, :, pl.ds(start, half)] = part[:, column : column + half]
    copy = pltpu.make_async_copy(whole, out.at[pl.ds(first, comps)], sem)
    copy.start()
    copy.wait()


def assemble_first(first, place, *refs):
    assemble(first, place, *refs[:-3], None, *refs[-3:])


def write_out(spots, parts, first, comps, shape, earlier):
    rows = parts[0].shape[0]
    smem, vmem, anywhere = (pl.BlockSpec(memory_space=m) for m in (pltpu.SMEM, pltpu.VMEM, pl.ANY))
    given = [] if earlier is None else [earlier]
    kernel = assemble if given else assemble_first
    return pl.pallas_call(
        lambda *refs: kernel(first, *refs),
        out_shape=jax.ShapeDtypeStruct(shape, jnp.bfloat16),
        in_specs=[smem] + [vmem] * len(parts) + [anywhere] * len(given),
        out_specs=anywhere,
        scratch_shapes=[pltpu.VMEM((comps, rows, shape[2]), jnp.bfloat16), pltpu.SemaphoreType.DMA],
        input_output_aliases={1 + len(parts): 0} if given else {},
        compiler_params=pltpu.CompilerParams(vmem_limit_bytes=8 << 20),
    )(spots, *parts, *given)


def direct(products, operator):
    points, comps, modes = products.shape
    flat = products.reshape(points, comps * modes)
    partial = jnp.dot(operator, flat, preferred_element_type=jnp.float32)
    summed = lax.psum_scatter(partial, "gy", scatter_dimension=0, tiled=True)
    result = summed.astype(jnp.bfloat16).reshape(points, comps, modes)
    return lax.all_to_all(result, "gx", split_axis=0, concat_axis=2, tiled=True)


def arrival_order(deep):
    return [0] + [k for k in list(range(deep - 1, 2, -1)) + [1, 2] if k < deep]


def paired(wide, deep, products, operator):
    points, comps, modes = products.shape
    chips, half = wide // 2, modes // 2
    piece = points // chips
    rows = piece // 2
    x, z = lax.axis_index("gx"), lax.axis_index("gy")
    chip, core, q = x // 2, x % 2, z % 2
    swap = [(i, i ^ 1) for i in range(wide)]
    order = arrival_order(deep)
    groups = [(0, half // 2), (half // 2, comps * half)]
    chunks = [(0, comps, [0, 1])]

    pieces = {
        k: lax.dynamic_slice_in_dim(operator, ((z ^ k) ^ core) * points + chip * piece, piece, 0) for k in order[1:]
    }
    products, pieces = lax.optimization_barrier((products, pieces))

    halves = [
        lax.dynamic_slice_in_dim(products, (q ^ odd) * half, half, 2).reshape(points, -1).T for odd in range(2)
    ]
    mine = []
    shares = {}
    for g, (a, b) in enumerate(groups):
        mine.append({0: halves[0][a:b]})
        for k in order[1:]:
            message = halves[k % 2][a:b]
            if g == 0:
                message = jnp.concatenate([pieces[k], message])
            message = lax.ppermute(message, "gy", [(i, i ^ k) for i in range(deep)])
            if g == 0:
                shares[k], message = message[:piece], message[piece:]
            mine[g][k] = message

    arrived = jnp.concatenate([shares[k] for k in range(1, deep)])
    gathered = [arrived]
    for j in range(1, chips):
        pairs = [(i, 2 * hop(i // 2, j, chips) + i % 2) for i in range(wide)]
        gathered.append(lax.ppermute(arrived, "gx", pairs))
    block = lax.dynamic_slice_in_dim(operator, (z ^ core) * points, points, 0)
    block = lax.optimization_barrier((block, arrived))[0]
    own = [lax.dynamic_slice_in_dim(block, back(chip, j, chips) * piece, piece, 0) for j in range(chips)]
    weights = [jnp.concatenate(own)]
    for k in range(deep - 1):
        weights.append(jnp.concatenate([g[k * piece : k * piece + piece] for g in gathered]))

    out = None
    for first, end, members in chunks:
        total = None
        for k in order:
            ours = jnp.concatenate([mine[g][k] for g in members])
            theirs = lax.ppermute(ours, "gx", swap)
            both = jnp.concatenate([ours, theirs])
            term = lax.dot_general(
                weights[k], both, (((1,), (1,)), ((), ())), preferred_element_type=jnp.float32
            )
            total = term if total is None else lax.optimization_barrier(total) + term
        result = total.astype(jnp.bfloat16).reshape(chips, piece, -1)

        kept, passed, places = [], [], []
        for j in list(range(1, chips)) + [0]:
            pairs = []
            for i in range(wide):
                for y in range(deep):
                    pairs.append((i * deep + y, (2 * back(i // 2, j, chips) + i % 2) * deep + (y ^ (i % 2))))
            landed = lax.ppermute(result[j], ("gx", "gy"), pairs)
            kept.append(lax.dynamic_slice_in_dim(landed, core * rows, rows, 0))
            passed.append(lax.dynamic_slice_in_dim(landed, (1 - core) * rows, rows, 0))
            places.append(hop(chip, j, chips))
        fetched = lax.ppermute(jnp.stack(passed), "gx", swap)
        spots = [
            (place * 2 + (core ^ via ^ e)) * 2 + (q ^ core ^ via)
            for via in range(2)
            for place in places
            for e in range(2)
        ]
        parts = kept + [fetched[i] for i in range(chips)]
        out = write_out(jnp.stack(spots).astype(jnp.int32), parts, first, end - first, (comps, rows, wide * modes), out)
    return out.transpose(1, 0, 2)


def solution(mesh):
    wide, deep = mesh.shape["gx"], mesh.shape["gy"]
    even = wide % 2 == 0 and deep > 1 and deep & (deep - 1) == 0

    def body(products, operator):
        if not even:
            return direct(products, operator)
        return paired(wide, deep, products, operator)

    return jax.shard_map(
        body,
        mesh=mesh,
        in_specs=(P("gy", None, "gx"), P(None, "gy")),
        out_specs=P(("gy", "gx"), None, None),
        check_vma=False,
    )
```

```python
import jax
import jax.numpy as jnp
from jax import lax
from jax.experimental import pallas as pl
from jax.experimental.pallas import tpu as pltpu
from jax.sharding import PartitionSpec as P


def hop(index, step, size):
    return index ^ step if size & (size - 1) == 0 else (index + step) % size


def back(index, step, size):
    return index ^ step if size & (size - 1) == 0 else (index - step + size) % size


def assemble(first, place, *refs):
    *parts, _, out, whole, sem = refs
    comps, _, width = whole.shape
    half = width // (2 * len(parts))
    for number, part in enumerate(parts):
        for other in range(2):
            start = pl.multiple_of(place[2 * number + other] * half, half)
            for comp in range(comps):
                column = (other * comps + comp) * half
                whole[comp, :, pl.ds(start, half)] = part[:, column : column + half]
    copy = pltpu.make_async_copy(whole, out.at[pl.ds(first, comps)], sem)
    copy.start()
    copy.wait()


def assemble_first(first, place, *refs):
    assemble(first, place, *refs[:-3], None, *refs[-3:])


def write_out(spots, parts, first, comps, shape, earlier):
    rows = parts[0].shape[0]
    smem, vmem, anywhere = (pl.BlockSpec(memory_space=m) for m in (pltpu.SMEM, pltpu.VMEM, pl.ANY))
    given = [] if earlier is None else [earlier]
    kernel = assemble if given else assemble_first
    return pl.pallas_call(
        lambda *refs: kernel(first, *refs),
        out_shape=jax.ShapeDtypeStruct(shape, jnp.bfloat16),
        in_specs=[smem] + [vmem] * len(parts) + [anywhere] * len(given),
        out_specs=anywhere,
        scratch_shapes=[pltpu.VMEM((comps, rows, shape[2]), jnp.bfloat16), pltpu.SemaphoreType.DMA],
        input_output_aliases={1 + len(parts): 0} if given else {},
        compiler_params=pltpu.CompilerParams(vmem_limit_bytes=8 << 20),
    )(spots, *parts, *given)


def direct(products, operator):
    points, comps, modes = products.shape
    flat = products.reshape(points, comps * modes)
    partial = jnp.dot(operator, flat, preferred_element_type=jnp.float32)
    summed = lax.psum_scatter(partial, "gy", scatter_dimension=0, tiled=True)
    result = summed.astype(jnp.bfloat16).reshape(points, comps, modes)
    return lax.all_to_all(result, "gx", split_axis=0, concat_axis=2, tiled=True)


def arrival_order(deep):
    return [0] + [k for k in list(range(deep - 1, 2, -1)) + [1, 2] if k < deep]


def paired(wide, deep, products, operator):
    points, comps, modes = products.shape
    chips, half = wide // 2, modes // 2
    piece = points // chips
    rows = piece // 2
    x, z = lax.axis_index("gx"), lax.axis_index("gy")
    chip, core, q = x // 2, x % 2, z % 2
    swap = [(i, i ^ 1) for i in range(wide)]
    order = arrival_order(deep)
    groups = [(0, half), (half, comps * half)]
    chunks = [(0, 1, [0]), (1, comps, [1])]

    pieces = {
        k: lax.dynamic_slice_in_dim(operator, ((z ^ k) ^ core) * points + chip * piece, piece, 0) for k in order[1:]
    }
    shares = {}
    for k in order[1:]:
        shares[k] = lax.ppermute(pieces[k], "gy", [(i, i ^ k) for i in range(deep)])

    halves = [
        lax.dynamic_slice_in_dim(products, (q ^ odd) * half, half, 2).reshape(points, -1).T for odd in range(2)
    ]
    mine = []
    for g, (a, b) in enumerate(groups):
        mine.append({0: halves[0][a:b]})
        for k in order[1:]:
            mine[g][k] = lax.ppermute(halves[k % 2][a:b], "gy", [(i, i ^ k) for i in range(deep)])

    arrived = jnp.concatenate([shares[k] for k in range(1, deep)])
    gathered = [arrived]
    for j in range(1, chips):
        pairs = [(i, 2 * hop(i // 2, j, chips) + i % 2) for i in range(wide)]
        gathered.append(lax.ppermute(arrived, "gx", pairs))
    block = lax.dynamic_slice_in_dim(operator, (z ^ core) * points, points, 0)
    block = lax.optimization_barrier((block, arrived))[0]
    own = [lax.dynamic_slice_in_dim(block, back(chip, j, chips) * piece, piece, 0) for j in range(chips)]
    weights = [jnp.concatenate(own)]
    for k in range(deep - 1):
        weights.append(jnp.concatenate([g[k * piece : k * piece + piece] for g in gathered]))

    out = None
    for first, end, members in chunks:
        total = None
        for k in order:
            ours = jnp.concatenate([mine[g][k] for g in members])
            theirs = lax.ppermute(ours, "gx", swap)
            both = jnp.concatenate([ours, theirs])
            term = lax.dot_general(
                weights[k], both, (((1,), (1,)), ((), ())), preferred_element_type=jnp.float32
            )
            total = term if total is None else lax.optimization_barrier(total) + term
        result = total.astype(jnp.bfloat16).reshape(chips, piece, -1)

        kept, passed, places = [], [], []
        for j in range(chips):
            pairs = []
            for i in range(wide):
                for y in range(deep):
                    pairs.append((i * deep + y, (2 * back(i // 2, j, chips) + i % 2) * deep + (y ^ (i % 2))))
            landed = lax.ppermute(result[j], ("gx", "gy"), pairs)
            kept.append(lax.dynamic_slice_in_dim(landed, core * rows, rows, 0))
            passed.append(lax.dynamic_slice_in_dim(landed, (1 - core) * rows, rows, 0))
            places.append(hop(chip, j, chips))
        fetched = lax.ppermute(jnp.stack(passed), "gx", swap)
        spots = [
            (place * 2 + (core ^ via ^ e)) * 2 + (q ^ core ^ via)
            for via in range(2)
            for place in places
            for e in range(2)
        ]
        parts = kept + [fetched[i] for i in range(chips)]
        out = write_out(jnp.stack(spots).astype(jnp.int32), parts, first, end - first, (comps, rows, wide * modes), out)
    return out.transpose(1, 0, 2)


def solution(mesh):
    wide, deep = mesh.shape["gx"], mesh.shape["gy"]
    even = wide % 2 == 0 and deep > 1 and deep & (deep - 1) == 0

    def body(products, operator):
        if not even:
            return direct(products, operator)
        return paired(wide, deep, products, operator)

    return jax.shard_map(
        body,
        mesh=mesh,
        in_specs=(P("gy", None, "gx"), P(None, "gy")),
        out_specs=P(("gy", "gx"), None, None),
        check_vma=False,
    )
```

```python
import functools

import jax
import jax.numpy as jnp
from jax import lax
from jax.experimental import pallas as pl
from jax.experimental.pallas import tpu as pltpu
from jax.sharding import PartitionSpec as P


def hop(index, step, size):
    return index ^ step if size & (size - 1) == 0 else (index + step) % size


def back(index, step, size):
    return index ^ step if size & (size - 1) == 0 else (index - step + size) % size


def assemble(chunks, place, *refs):
    *kept, fetched, out = refs
    many = len(kept) // len(chunks)
    half = out.shape[2] // (4 * many)

    def put(spot, comp, values):
        out[comp, :, pl.ds(pl.multiple_of(place[spot] * half, half), half)] = values

    for c, (first, end) in enumerate(chunks):
        for number in range(many):
            for other in range(2):
                for comp in range(first, end):
                    column = (other * (end - first) + comp - first) * half
                    put(2 * number + other, comp, kept[c * many + number][:, column : column + half])
                    column += 2 * first * half
                    put(2 * (many + number) + other, comp, fetched[number, :, column : column + half])


def direct(products, operator):
    points, comps, modes = products.shape
    flat = products.reshape(points, comps * modes)
    partial = jnp.dot(operator, flat, preferred_element_type=jnp.float32)
    summed = lax.psum_scatter(partial, "gy", scatter_dimension=0, tiled=True)
    result = summed.astype(jnp.bfloat16).reshape(points, comps, modes)
    return lax.all_to_all(result, "gx", split_axis=0, concat_axis=2, tiled=True)


def arrival_order(deep):
    return [0] + [k for k in list(range(deep - 1, 2, -1)) + [1, 2] if k < deep]


def paired(wide, deep, products, operator):
    points, comps, modes = products.shape
    chips, half = wide // 2, modes // 2
    piece = points // chips
    rows = piece // 2
    x, z = lax.axis_index("gx"), lax.axis_index("gy")
    chip, core, q = x // 2, x % 2, z % 2
    swap = [(i, i ^ 1) for i in range(wide)]
    order = arrival_order(deep)
    groups = [(0, half), (half, comps * half)]
    chunks = [(0, 1, [0]), (1, comps, [1])]

    pieces = {
        k: lax.dynamic_slice_in_dim(operator, ((z ^ k) ^ core) * points + chip * piece, piece, 0) for k in order[1:]
    }
    shares = {}
    for k in order[1:]:
        shares[k] = lax.ppermute(pieces[k], "gy", [(i, i ^ k) for i in range(deep)])

    halves = [
        lax.dynamic_slice_in_dim(products, (q ^ odd) * half, half, 2).reshape(points, -1).T for odd in range(2)
    ]
    mine = []
    for g, (a, b) in enumerate(groups):
        mine.append({0: halves[0][a:b]})
        for k in order[1:]:
            mine[g][k] = lax.ppermute(halves[k % 2][a:b], "gy", [(i, i ^ k) for i in range(deep)])

    arrived = jnp.concatenate([shares[k] for k in range(1, deep)])
    gathered = [arrived]
    for j in range(1, chips):
        pairs = [(i, 2 * hop(i // 2, j, chips) + i % 2) for i in range(wide)]
        gathered.append(lax.ppermute(arrived, "gx", pairs))
    block = lax.dynamic_slice_in_dim(operator, (z ^ core) * points, points, 0)
    block = lax.optimization_barrier((block, arrived))[0]
    own = [lax.dynamic_slice_in_dim(block, back(chip, j, chips) * piece, piece, 0) for j in range(chips)]
    weights = [jnp.concatenate(own)]
    for k in range(deep - 1):
        weights.append(jnp.concatenate([g[k * piece : k * piece + piece] for g in gathered]))

    kept, passed = [], []
    for first, end, members in chunks:
        total = None
        for k in order:
            ours = jnp.concatenate([mine[g][k] for g in members])
            theirs = lax.ppermute(ours, "gx", swap)
            both = jnp.concatenate([ours, theirs])
            term = lax.dot_general(
                weights[k], both, (((1,), (1,)), ((), ())), preferred_element_type=jnp.float32
            )
            total = term if total is None else lax.optimization_barrier(total) + term
        result = total.astype(jnp.bfloat16).reshape(chips, piece, -1)

        for j in range(chips):
            pairs = []
            for i in range(wide):
                for y in range(deep):
                    pairs.append((i * deep + y, (2 * back(i // 2, j, chips) + i % 2) * deep + (y ^ (i % 2))))
            landed = lax.ppermute(result[j], ("gx", "gy"), pairs)
            kept.append(lax.dynamic_slice_in_dim(landed, core * rows, rows, 0))
            passed.append(lax.dynamic_slice_in_dim(landed, (1 - core) * rows, rows, 0))
    passed = [jnp.concatenate(passed[j::chips], axis=1) for j in range(chips)]
    fetched = lax.ppermute(jnp.stack(passed), "gx", swap)
    spots = [
        (hop(chip, j, chips) * 2 + (core ^ via ^ e)) * 2 + (q ^ core ^ via)
        for via in range(2)
        for j in range(chips)
        for e in range(2)
    ]
    smem, vmem = (pl.BlockSpec(memory_space=m) for m in (pltpu.SMEM, pltpu.VMEM))
    out = pl.pallas_call(
        functools.partial(assemble, [chunk[:2] for chunk in chunks]),
        out_shape=jax.ShapeDtypeStruct((comps, rows, wide * modes), jnp.bfloat16),
        in_specs=[smem] + [vmem] * (len(kept) + 1),
        out_specs=vmem,
        compiler_params=pltpu.CompilerParams(vmem_limit_bytes=8 << 20),
    )(jnp.stack(spots).astype(jnp.int32), *kept, fetched)
    return out.transpose(1, 0, 2)


def solution(mesh):
    wide, deep = mesh.shape["gx"], mesh.shape["gy"]
    even = wide % 2 == 0 and deep > 1 and deep & (deep - 1) == 0

    def body(products, operator):
        if not even:
            return direct(products, operator)
        return paired(wide, deep, products, operator)

    return jax.shard_map(
        body,
        mesh=mesh,
        in_specs=(P("gy", None, "gx"), P(None, "gy")),
        out_specs=P(("gy", "gx"), None, None),
        check_vma=False,
    )
```

```python
import functools

import jax
import jax.numpy as jnp
from jax import lax
from jax.experimental import pallas as pl
from jax.experimental.pallas import tpu as pltpu
from jax.sharding import PartitionSpec as P


def hop(index, step, size):
    return index ^ step if size & (size - 1) == 0 else (index + step) % size


def back(index, step, size):
    return index ^ step if size & (size - 1) == 0 else (index - step + size) % size


def assemble(chunks, *refs):
    *kept, fetched, out, whole, sems = refs
    many = len(kept) // len(chunks)
    x, z = lax.axis_index("gx"), lax.axis_index("gy")
    chip, core, q = lax.div(x, 2), lax.rem(x, 2), lax.rem(z, 2)
    place = [
        (hop(chip, j, many) * 2 + (core ^ via ^ e)) * 2 + (q ^ core ^ via)
        for via in range(2)
        for j in range(many)
        for e in range(2)
    ]
    half = whole.shape[2] // (4 * many)
    copies = []
    for c, (first, end) in enumerate(chunks):
        for comp in range(first, end):
            for number in range(many):
                for other in range(2):
                    column = (other * (end - first) + comp - first) * half
                    beside = column + 2 * first * half
                    for spot, values in (
                        (2 * number + other, kept[c * many + number][:, column : column + half]),
                        (2 * (many + number) + other, fetched[number, :, beside : beside + half]),
                    ):
                        whole[comp, :, pl.ds(pl.multiple_of(place[spot] * half, half), half)] = values
            copies.append(pltpu.make_async_copy(whole.at[comp], out.at[comp], sems.at[comp]))
            copies[-1].start()
    for copy in copies:
        copy.wait()


def direct(products, operator):
    points, comps, modes = products.shape
    flat = products.reshape(points, comps * modes)
    partial = jnp.dot(operator, flat, preferred_element_type=jnp.float32)
    summed = lax.psum_scatter(partial, "gy", scatter_dimension=0, tiled=True)
    result = summed.astype(jnp.bfloat16).reshape(points, comps, modes)
    return lax.all_to_all(result, "gx", split_axis=0, concat_axis=2, tiled=True)


def arrival_order(deep):
    return [0] + [k for k in list(range(deep - 1, 2, -1)) + [1, 2] if k < deep]


def paired(wide, deep, products, operator):
    points, comps, modes = products.shape
    chips, half = wide // 2, modes // 2
    piece = points // chips
    rows = piece // 2
    x, z = lax.axis_index("gx"), lax.axis_index("gy")
    chip, core, q = x // 2, x % 2, z % 2
    swap = [(i, i ^ 1) for i in range(wide)]
    order = arrival_order(deep)
    groups = [(0, half), (half, comps * half)]
    chunks = [(0, 1, [0]), (1, comps, [1])]

    pieces = {
        k: lax.dynamic_slice_in_dim(operator, ((z ^ k) ^ core) * points + chip * piece, piece, 0) for k in order[1:]
    }
    shares = {}
    for k in order[1:]:
        shares[k] = lax.ppermute(pieces[k], "gy", [(i, i ^ k) for i in range(deep)])

    halves = [
        lax.dynamic_slice_in_dim(products, (q ^ odd) * half, half, 2).reshape(points, -1).T for odd in range(2)
    ]
    mine = []
    for g, (a, b) in enumerate(groups):
        mine.append({0: halves[0][a:b]})
        for k in order[1:]:
            mine[g][k] = lax.ppermute(halves[k % 2][a:b], "gy", [(i, i ^ k) for i in range(deep)])

    arrived = jnp.concatenate([shares[k] for k in range(1, deep)])
    gathered = [arrived]
    for j in range(1, chips):
        pairs = [(i, 2 * hop(i // 2, j, chips) + i % 2) for i in range(wide)]
        gathered.append(lax.ppermute(arrived, "gx", pairs))
    block = lax.dynamic_slice_in_dim(operator, (z ^ core) * points, points, 0)
    block = lax.optimization_barrier((block, arrived))[0]
    own = [lax.dynamic_slice_in_dim(block, back(chip, j, chips) * piece, piece, 0) for j in range(chips)]
    weights = [jnp.concatenate(own)]
    for k in range(deep - 1):
        weights.append(jnp.concatenate([g[k * piece : k * piece + piece] for g in gathered]))

    kept, passed = [], []
    for first, end, members in chunks:
        total = None
        for k in order:
            ours = jnp.concatenate([mine[g][k] for g in members])
            theirs = lax.ppermute(ours, "gx", swap)
            both = jnp.concatenate([ours, theirs])
            term = lax.dot_general(
                weights[k], both, (((1,), (1,)), ((), ())), preferred_element_type=jnp.float32
            )
            total = term if total is None else lax.optimization_barrier(total) + term
        result = total.astype(jnp.bfloat16).reshape(chips, piece, -1)

        for j in range(chips):
            pairs = []
            for i in range(wide):
                for y in range(deep):
                    pairs.append((i * deep + y, (2 * back(i // 2, j, chips) + i % 2) * deep + (y ^ (i % 2))))
            landed = lax.ppermute(result[j], ("gx", "gy"), pairs)
            kept.append(lax.dynamic_slice_in_dim(landed, core * rows, rows, 0))
            passed.append(lax.dynamic_slice_in_dim(landed, (1 - core) * rows, rows, 0))
    passed = [jnp.concatenate(passed[j::chips], axis=1) for j in range(chips)]
    fetched = lax.ppermute(jnp.stack(passed), "gx", swap)
    vmem = pl.BlockSpec(memory_space=pltpu.VMEM)
    out = pl.pallas_call(
        functools.partial(assemble, [chunk[:2] for chunk in chunks]),
        out_shape=jax.ShapeDtypeStruct((comps, rows, wide * modes), jnp.bfloat16),
        in_specs=[vmem] * (len(kept) + 1),
        out_specs=pl.BlockSpec(memory_space=pl.ANY),
        scratch_shapes=[
            pltpu.VMEM((comps, rows, wide * modes), jnp.bfloat16),
            pltpu.SemaphoreType.DMA((comps,)),
        ],
        compiler_params=pltpu.CompilerParams(vmem_limit_bytes=8 << 20),
    )(*kept, fetched)
    return out.transpose(1, 0, 2)


def solution(mesh):
    wide, deep = mesh.shape["gx"], mesh.shape["gy"]
    even = wide % 2 == 0 and deep > 1 and deep & (deep - 1) == 0

    def body(products, operator):
        if not even:
            return direct(products, operator)
        return paired(wide, deep, products, operator)

    return jax.shard_map(
        body,
        mesh=mesh,
        in_specs=(P("gy", None, "gx"), P(None, "gy")),
        out_specs=P(("gy", "gx"), None, None),
        check_vma=False,
    )
```

```python
import functools

import jax
import jax.numpy as jnp
from jax import lax
from jax.experimental import pallas as pl
from jax.experimental.pallas import tpu as pltpu
from jax.sharding import PartitionSpec as P


def hop(index, step, size):
    return index ^ step if size & (size - 1) == 0 else (index + step) % size


def back(index, step, size):
    return index ^ step if size & (size - 1) == 0 else (index - step + size) % size


def assemble(chunks, *refs):
    *kept, fetched, out, whole, sems = refs
    many = len(kept) // len(chunks)
    x, z = lax.axis_index("gx"), lax.axis_index("gy")
    chip, core, q = lax.div(x, 2), lax.rem(x, 2), lax.rem(z, 2)
    place = [
        (hop(chip, j, many) * 2 + (core ^ via ^ e)) * 2 + (q ^ core ^ via)
        for via in range(2)
        for j in range(many)
        for e in range(2)
    ]
    half = whole.shape[2] // (4 * many)
    copies = []
    for c, (first, end) in enumerate(chunks):
        for comp in range(first, end):
            for number in range(many):
                for other in range(2):
                    column = (other * (end - first) + comp - first) * half
                    beside = column + 2 * first * half
                    for spot, values in (
                        (2 * number + other, kept[c * many + number][:, column : column + half]),
                        (2 * (many + number) + other, fetched[number, :, beside : beside + half]),
                    ):
                        whole[comp, :, pl.ds(pl.multiple_of(place[spot] * half, half), half)] = values
            copies.append(pltpu.make_async_copy(whole.at[comp], out.at[comp], sems.at[comp]))
            copies[-1].start()
    for copy in copies:
        copy.wait()


def direct(products, operator):
    points, comps, modes = products.shape
    flat = products.reshape(points, comps * modes)
    partial = jnp.dot(operator, flat, preferred_element_type=jnp.float32)
    summed = lax.psum_scatter(partial, "gy", scatter_dimension=0, tiled=True)
    result = summed.astype(jnp.bfloat16).reshape(points, comps, modes)
    return lax.all_to_all(result, "gx", split_axis=0, concat_axis=2, tiled=True)


def arrival_order(deep):
    return [0] + [k for k in list(range(deep - 1, 2, -1)) + [1, 2] if k < deep]


def swap_waves(deep, chunk):
    own, *ks = arrival_order(deep)
    waves = [[own], ks] if chunk == 0 else [[own]] + [[k] for k in ks]
    return [wave for wave in waves if wave]


def paired(wide, deep, products, operator):
    points, comps, modes = products.shape
    chips, half = wide // 2, modes // 2
    piece = points // chips
    rows = piece // 2
    x, z = lax.axis_index("gx"), lax.axis_index("gy")
    chip, core, q = x // 2, x % 2, z % 2
    swap = [(i, i ^ 1) for i in range(wide)]
    order = arrival_order(deep)
    groups = [(0, half), (half, comps * half)]
    chunks = [(0, 1, [0]), (1, comps, [1])]

    pieces = {
        k: lax.dynamic_slice_in_dim(operator, ((z ^ k) ^ core) * points + chip * piece, piece, 0) for k in order[1:]
    }
    shares = {}
    for k in order[1:]:
        shares[k] = lax.ppermute(pieces[k], "gy", [(i, i ^ k) for i in range(deep)])

    halves = [
        lax.dynamic_slice_in_dim(products, (q ^ odd) * half, half, 2).reshape(points, -1).T for odd in range(2)
    ]
    mine = []
    for g, (a, b) in enumerate(groups):
        mine.append({0: halves[0][a:b]})
        for k in order[1:]:
            mine[g][k] = lax.ppermute(halves[k % 2][a:b], "gy", [(i, i ^ k) for i in range(deep)])

    arrived = jnp.concatenate([shares[k] for k in range(1, deep)])
    gathered = [arrived]
    for j in range(1, chips):
        pairs = [(i, 2 * hop(i // 2, j, chips) + i % 2) for i in range(wide)]
        gathered.append(lax.ppermute(arrived, "gx", pairs))
    block = lax.dynamic_slice_in_dim(operator, (z ^ core) * points, points, 0)
    block = lax.optimization_barrier((block, arrived))[0]
    own = [lax.dynamic_slice_in_dim(block, back(chip, j, chips) * piece, piece, 0) for j in range(chips)]
    weights = [jnp.concatenate(own)]
    for k in range(deep - 1):
        weights.append(jnp.concatenate([g[k * piece : k * piece + piece] for g in gathered]))

    kept, passed = [], []
    for c, (first, end, members) in enumerate(chunks):
        total = None
        ours = {k: jnp.concatenate([mine[g][k] for g in members]) for k in order}
        theirs = {}
        for wave in swap_waves(deep, c):
            swapped = lax.ppermute(jnp.concatenate([ours[k] for k in wave]), "gx", swap)
            for k, part in zip(wave, jnp.split(swapped, len(wave))):
                theirs[k] = part
        for k in order:
            both = jnp.concatenate([ours[k], theirs[k]])
            term = lax.dot_general(
                weights[k], both, (((1,), (1,)), ((), ())), preferred_element_type=jnp.float32
            )
            total = term if total is None else lax.optimization_barrier(total) + term
        result = total.astype(jnp.bfloat16).reshape(chips, piece, -1)

        for j in range(chips):
            pairs = []
            for i in range(wide):
                for y in range(deep):
                    pairs.append((i * deep + y, (2 * back(i // 2, j, chips) + i % 2) * deep + (y ^ (i % 2))))
            landed = lax.ppermute(result[j], ("gx", "gy"), pairs)
            kept.append(lax.dynamic_slice_in_dim(landed, core * rows, rows, 0))
            passed.append(lax.dynamic_slice_in_dim(landed, (1 - core) * rows, rows, 0))
    passed = [jnp.concatenate(passed[j::chips], axis=1) for j in range(chips)]
    fetched = lax.ppermute(jnp.stack(passed), "gx", swap)
    vmem = pl.BlockSpec(memory_space=pltpu.VMEM)
    out = pl.pallas_call(
        functools.partial(assemble, [chunk[:2] for chunk in chunks]),
        out_shape=jax.ShapeDtypeStruct((comps, rows, wide * modes), jnp.bfloat16),
        in_specs=[vmem] * (len(kept) + 1),
        out_specs=pl.BlockSpec(memory_space=pl.ANY),
        scratch_shapes=[
            pltpu.VMEM((comps, rows, wide * modes), jnp.bfloat16),
            pltpu.SemaphoreType.DMA((comps,)),
        ],
        compiler_params=pltpu.CompilerParams(vmem_limit_bytes=8 << 20),
    )(*kept, fetched)
    return out.transpose(1, 0, 2)


def solution(mesh):
    wide, deep = mesh.shape["gx"], mesh.shape["gy"]
    even = wide % 2 == 0 and deep > 1 and deep & (deep - 1) == 0

    def body(products, operator):
        if not even:
            return direct(products, operator)
        return paired(wide, deep, products, operator)

    return jax.shard_map(
        body,
        mesh=mesh,
        in_specs=(P("gy", None, "gx"), P(None, "gy")),
        out_specs=P(("gy", "gx"), None, None),
        check_vma=False,
    )
```
